32 devices in a mesh: seq: 8 (over z, y), head: 4 (over x, core).
Axes of the slice: x: 2, y: 2, z: 4, core: 2. Of those that a mesh axis runs over, the one named last changes fastest.
Arguments:
- queries: bfloat16 [4096, 8192], P(('seq', 'head')), may hold values from -8 to 8
- keys: bfloat16 [4096, 1024], P(('seq', 'head')), may hold values from -8 to 8
- values: bfloat16 [4096, 1024], P(('seq', 'head')), may hold values from -6 to 6
- selected: int32 [32, 8], P('seq'), may hold values from 0 to 31, as said below
- counts: int32 [32], P('seq'), may hold values from 1 to 8
- block_slot: int32 [32], P('seq'), may hold values from 0 to 31, as said below
Outputs:
- attended: bfloat16 [4096, 8192], P(('seq', 'head'))
The draws below stay inside these ranges and needn't reach their ends.
Inputs may be any that keep to these rules, and one draw needn't show every extreme that they name: A permutation of 0 to 31. Block b's rows of keys and values start at row 128 * block_slot[b]; its owner shard is block_slot[b] // 4. The 4 blocks of one sequence shard (blocks s * 4 onward) have distinct owner shards, and block_slot[b] % 4 == b % 4. `selected`: row q lists its live entries first: entry 0 is q itself, the other live entries are distinct blocks of earlier sequence shards; entries from counts[q] on are 0. Over the live entries of the 4 rows of one sequence shard, at most 2 distinct blocks have the same owner shard, and in every draw some shard reaches 2 from some owner.
All inputs are finite; a program needn't handle non-finite values.
Results may differ from the reference program's by a relative error of at most 0.0049.
Values may be sent and summed in bfloat16 or wider, within the bound.
No kernel may reach another device: no remote copies, remote signals or barrier semaphores. Data moves between devices by JAX's collectives and lax.ppermute only.
A program may use at most 128 MiB of HBM per device.

```python
import math
import jax
import jax.numpy as jnp
from jax import lax

QUERY_HEADS = 64
KEY_VALUE_HEADS = 8
HEAD_SIZE = 128
BLOCK_ROWS = 128
SELECTION_COUNT = 8
BLK_SEQ = 4
NB = 32
TOKEN_COUNT = 4096
N_SEQ = 8


def selection_tables(key):
    base = jax.random.fold_in(key, 4049)
    keys_list = jax.random.split(base, 5)
    shard_perm = jax.random.permutation(keys_list[0], N_SEQ).astype(jnp.int32)
    offsets = jax.random.permutation(keys_list[1], N_SEQ)[:BLK_SEQ].astype(jnp.int32)
    blocks = jnp.arange(NB, dtype=jnp.int32)
    home_shard = blocks // BLK_SEQ
    within = blocks % BLK_SEQ
    owner_of = (shard_perm[home_shard] + offsets[within]) % N_SEQ
    slot_of = owner_of * BLK_SEQ + within
    by_slot = jnp.zeros((NB,), jnp.int32).at[slot_of].set(blocks)
    slot_grid = by_slot.reshape(N_SEQ, BLK_SEQ)
    grid_shard = slot_grid // BLK_SEQ
    rank_draw = jax.random.randint(keys_list[2], (N_SEQ, N_SEQ, BLK_SEQ), 0, 1 << 20) * BLK_SEQ + jnp.arange(BLK_SEQ, dtype=jnp.int32)
    requesters = jnp.arange(N_SEQ, dtype=jnp.int32)[:, None, None]
    masked = jnp.where(grid_shard[None] < requesters, rank_draw, -1)
    best_pick = jnp.argmax(masked, axis=2).astype(jnp.int32)
    extra_ok = jnp.max(masked, axis=2) >= 0
    spread_grid = jnp.broadcast_to(slot_grid[None], (N_SEQ, N_SEQ, BLK_SEQ))
    extra_block = jnp.take_along_axis(spread_grid, best_pick[:, :, None], axis=2)[:, :, 0]
    priority = jax.random.randint(keys_list[3], (NB, N_SEQ), 0, 1 << 20) * N_SEQ + jnp.arange(N_SEQ, dtype=jnp.int32)[None, :]
    first_owner = owner_of[home_shard * BLK_SEQ]
    forced = (within == BLK_SEQ - 1)[:, None] & (jnp.arange(N_SEQ, dtype=jnp.int32)[None, :] == first_owner[:, None])
    priority = jnp.where(forced, 1 << 30, priority)
    usable = extra_ok[home_shard]
    priority = jnp.where(usable, priority, -1)
    top_values, top_index = lax.top_k(priority, SELECTION_COUNT - 1)
    picked = jnp.take_along_axis(extra_block[home_shard], top_index, axis=1)
    pool_size = jnp.sum(usable.astype(jnp.int32), axis=1)
    want_count = jax.random.randint(keys_list[4], (NB,), SELECTION_COUNT // 2, SELECTION_COUNT)
    extra_count = jnp.minimum(want_count, pool_size).astype(jnp.int32)
    position = jnp.arange(SELECTION_COUNT - 1, dtype=jnp.int32)[None, :]
    picked = jnp.where(position < extra_count[:, None], picked, 0).astype(jnp.int32)
    chosen = jnp.concatenate([blocks[:, None], picked], axis=1).astype(jnp.int32)
    return (slot_of.astype(jnp.int32), chosen, (1 + extra_count).astype(jnp.int32))


def draw_selected(key, part):
    return selection_tables(key)[1]


def draw_counts(key, part):
    return selection_tables(key)[2]


def draw_block_slot(key, part):
    return selection_tables(key)[0]


def draw_queries(key, part):
    random_portion = jax.random.normal(jax.random.fold_in(key, 11), (TOKEN_COUNT, QUERY_HEADS, HEAD_SIZE), jnp.float32)
    sampled_blocks = random_portion
    return jnp.clip(sampled_blocks, -8.0, 8.0).reshape(TOKEN_COUNT, QUERY_HEADS * HEAD_SIZE).astype(jnp.bfloat16)


def draw_keys(key, part):
    random_portion = jax.random.normal(jax.random.fold_in(key, 21), (TOKEN_COUNT, KEY_VALUE_HEADS, HEAD_SIZE), jnp.float32)
    sampled_blocks = random_portion
    return jnp.clip(sampled_blocks, -8.0, 8.0).reshape(TOKEN_COUNT, KEY_VALUE_HEADS * HEAD_SIZE).astype(jnp.bfloat16)


def shard_levels(stream_key, dims, pieces, least, largest):
    def one(dim, shards_of):
        heights = jax.random.uniform(jax.random.fold_in(jax.random.fold_in(stream_key, 6), dim), (shards_of,), jnp.float32, least / len(pieces), largest / len(pieces))
        return jnp.repeat(jnp.exp(heights), dims[dim] // shards_of).reshape((-1,) + (1,) * (len(dims) - dim - 1))

    level = one(*pieces[0])
    for cut in pieces[1:]:
        level = level * one(*cut)
    return level


def centred(key, dims, width, limit, cuts=(), kind=jnp.bfloat16):
    gain = shard_levels(key, dims, cuts, -0.22, 0.18) if cuts else 1.0
    entries = jax.random.normal(key, dims, jnp.float32) * width * gain
    return jnp.minimum(jnp.maximum(entries, -limit), limit).astype(kind)


def setup_inputs(seed: int = 0) -> dict:
    splits = jax.random.split(jax.random.key(seed), 7)
    queries = draw_queries(jax.random.fold_in(splits[6], 71), 0)
    keys = draw_keys(jax.random.fold_in(splits[6], 71), 0)
    values = centred(splits[2], (TOKEN_COUNT, KEY_VALUE_HEADS * HEAD_SIZE), 1.0, 6.0, ((0, 32),))
    selected = draw_selected(jax.random.fold_in(splits[6], 71), 0)
    counts = draw_counts(jax.random.fold_in(splits[6], 71), 0)
    block_slot = draw_block_slot(jax.random.fold_in(splits[6], 71), 0)
    return dict(queries=queries, keys=keys, values=values, selected=selected, counts=counts, block_slot=block_slot)


def reference(queries, keys, values, selected, counts, block_slot):
    block_count = selected.shape[0]
    heads_per_group = QUERY_HEADS // KEY_VALUE_HEADS
    score_scale = 1.0 / math.sqrt(HEAD_SIZE)
    key_block_list = keys.reshape(block_count, BLOCK_ROWS, KEY_VALUE_HEADS, HEAD_SIZE)
    value_block_list = values.reshape(block_count, BLOCK_ROWS, KEY_VALUE_HEADS, HEAD_SIZE)
    query_block_list = queries.reshape(block_count, BLOCK_ROWS, KEY_VALUE_HEADS, heads_per_group, HEAD_SIZE)

    def one_block(operands):
        block_id, query_tile, chosen, live_count = operands
        holder_shard = block_slot[chosen]
        key_block_rows = key_block_list[holder_shard].reshape(SELECTION_COUNT * BLOCK_ROWS, KEY_VALUE_HEADS, HEAD_SIZE)
        value_block_rows = value_block_list[holder_shard].reshape(SELECTION_COUNT * BLOCK_ROWS, KEY_VALUE_HEADS, HEAD_SIZE)
        scores = jnp.einsum('igmd,kgd->gmik', query_tile.astype(jnp.float32), key_block_rows.astype(jnp.float32)) * score_scale
        query_pos = block_id * BLOCK_ROWS + jnp.arange(BLOCK_ROWS, dtype=jnp.int32)
        key_pos = (chosen[:, None] * BLOCK_ROWS + jnp.arange(BLOCK_ROWS, dtype=jnp.int32)[None, :]).reshape(-1)
        live_entry = jnp.repeat(jnp.arange(SELECTION_COUNT, dtype=jnp.int32) < live_count, BLOCK_ROWS)
        visible = live_entry[None, :] & (key_pos[None, :] <= query_pos[:, None])
        scores = jnp.where(visible[None, None], scores, -jnp.inf)
        row_top = lax.optimization_barrier(jnp.max(scores, axis=-1, keepdims=True))
        weights = jnp.exp(scores - row_top)
        probability = (weights / lax.optimization_barrier(jnp.sum(weights, axis=-1, keepdims=True))).astype(jnp.bfloat16)
        mixed_out = jnp.einsum('gmik,kgd->igmd', probability.astype(jnp.float32), value_block_rows.astype(jnp.float32))
        return mixed_out.astype(jnp.bfloat16).reshape(BLOCK_ROWS, QUERY_HEADS * HEAD_SIZE)
    attended = lax.map(one_block, (jnp.arange(block_count, dtype=jnp.int32), query_block_list, selected, counts))
    return attended.reshape(block_count * BLOCK_ROWS, QUERY_HEADS * HEAD_SIZE)
```

```python
import math

import jax
import jax.numpy as jnp
from jax import lax
from jax.experimental import pallas as pl
from jax.experimental.pallas import tpu as pltpu
from jax.sharding import Mesh
from jax.sharding import PartitionSpec as P

KV_HEADS = 8
HEAD_SIZE = 128
BLOCK_ROWS = 128
SELECTION_COUNT = 8
CHAIN_MAX = 4
NEG = -1e30


def attend_kernel(tab_ref, q_ref, kv_ref, o_ref, s_ref, *, d, groups):
    rows = groups * BLOCK_ROWS
    count = tab_ref[d, 0]
    pairs = (count + 1) // 2
    q = jnp.concatenate(
        [q_ref[:, m * HEAD_SIZE : (m + 1) * HEAD_SIZE] for m in range(groups)], axis=0
    )
    contract = (((1,), (1,)), ((), ()))

    def keys_of(p, which):
        a = kv_ref[tab_ref[d, 1 + 2 * p], which]
        b = kv_ref[tab_ref[d, 2 + 2 * p], which]
        return jnp.concatenate([a, b], axis=0)

    def scores(p):
        s = lax.dot_general(q, keys_of(p, 0), contract, preferred_element_type=jnp.float32)
        live = 2 * p + 1 < count
        sa = s[:, :BLOCK_ROWS]
        sb = jnp.where(live, s[:, BLOCK_ROWS:], NEG)
        return sa, sb

    sa, sb = scores(0)
    qpos = lax.broadcasted_iota(jnp.int32, (BLOCK_ROWS, BLOCK_ROWS), 0)
    kpos = lax.broadcasted_iota(jnp.int32, (BLOCK_ROWS, BLOCK_ROWS), 1)
    tri = kpos <= qpos
    sa = jnp.where(tri[None], sa.reshape(groups, BLOCK_ROWS, BLOCK_ROWS), NEG)
    sa = sa.reshape(rows, BLOCK_ROWS)
    s_ref[0, :, :BLOCK_ROWS] = sa
    s_ref[0, :, BLOCK_ROWS:] = sb
    top = jnp.maximum(sa, sb)

    def score_step(p, top):
        sa, sb = scores(p)
        s_ref[p, :, :BLOCK_ROWS] = sa
        s_ref[p, :, BLOCK_ROWS:] = sb
        return jnp.maximum(top, jnp.maximum(sa, sb))

    top = lax.fori_loop(1, pairs, score_step, top)
    c = math.log2(math.e) / math.sqrt(HEAD_SIZE)
    shift = jnp.max(top, axis=1, keepdims=True) * c
    ones = jnp.ones((2 * BLOCK_ROWS, HEAD_SIZE), jnp.bfloat16)

    def mix(p):
        w = jnp.exp2(s_ref[p] * c - shift).astype(jnp.bfloat16)
        ve = jnp.concatenate([keys_of(p, 1), ones], axis=1)
        return jnp.dot(w, ve, preferred_element_type=jnp.float32)

    acc = lax.fori_loop(1, pairs, lambda p, acc: acc + mix(p), mix(0))
    out = (acc[:, :HEAD_SIZE] / acc[:, HEAD_SIZE:]).astype(jnp.bfloat16)
    for m in range(groups):
        o_ref[:, m * HEAD_SIZE : (m + 1) * HEAD_SIZE] = out[m * BLOCK_ROWS : (m + 1) * BLOCK_ROWS]


def attend(table, q, kv, d, groups):
    import functools

    return pl.pallas_call(
        functools.partial(attend_kernel, d=d, groups=groups),
        out_shape=jax.ShapeDtypeStruct(q.shape, q.dtype),
        in_specs=[
            pl.BlockSpec(memory_space=pltpu.SMEM),
            pl.BlockSpec(memory_space=pltpu.VMEM),
            pl.BlockSpec(memory_space=pltpu.VMEM),
        ],
        out_specs=pl.BlockSpec(memory_space=pltpu.VMEM),
        scratch_shapes=[
            pltpu.VMEM(
                (SELECTION_COUNT // 2, groups * BLOCK_ROWS, 2 * BLOCK_ROWS), jnp.float32
            )
        ],
        name="attend",
    )(table, q, kv)


def place_kernel(me_ref, *refs):
    n = len(refs) - 2
    out, sems = refs[n], refs[n + 1]
    width = refs[0].shape[1]
    copies = []
    for d in range(n):
        col = pl.multiple_of((me_ref[0] ^ d) * width, width)
        copies.append(pltpu.make_async_copy(refs[d], out.at[:, pl.ds(col, width)], sems.at[d]))
    for c in copies:
        c.start()
    for c in copies:
        c.wait()


def place(me, parts):
    n = len(parts)
    rows, width = parts[0].shape
    return pl.pallas_call(
        place_kernel,
        out_shape=jax.ShapeDtypeStruct((rows, n * width), parts[0].dtype),
        in_specs=[pl.BlockSpec(memory_space=pltpu.SMEM)]
        + [pl.BlockSpec(memory_space=pl.ANY)] * n,
        out_specs=pl.BlockSpec(memory_space=pl.ANY),
        scratch_shapes=[pltpu.SemaphoreType.DMA((n,))],
        name="place",
    )(me.reshape(1), *parts)


def body(queries, keys, values, selected, counts, block_slot):
    plane = ("y", "head")
    nz = lax.axis_size("z")
    ny = lax.axis_size("y")
    nh = lax.axis_size("head")
    n = ny * nh
    z = lax.axis_index("z")
    me = lax.axis_index("y") * nh + lax.axis_index("head")
    width = queries.shape[1] // n
    groups = width // HEAD_SIZE
    blk_seq = selected.shape[0]

    def split(x):
        return x.reshape(BLOCK_ROWS, n, HEAD_SIZE).transpose(1, 0, 2)

    kv = jnp.stack([split(keys), split(values)], axis=1)
    kv = lax.all_to_all(kv, plane, split_axis=0, concat_axis=0, tiled=True)

    q_parts = []
    for d in range(n):
        part = lax.dynamic_slice_in_dim(queries, (me ^ d) * width, width, axis=1)
        if d:
            part = lax.ppermute(part, plane, [(s, s ^ d) for s in range(n)])
        q_parts.append(part)

    mine = jnp.concatenate([selected, counts[:, None], block_slot[:, None]], axis=1)
    shards = nz * ny
    everyone = lax.all_to_all(
        jnp.broadcast_to(mine[None], (shards,) + mine.shape),
        ("z", "y"), split_axis=0, concat_axis=0, tiled=True,
    )
    slots = everyone[:, :, SELECTION_COUNT + 1].reshape(-1)

    if nz <= CHAIN_MAX:
        up, down = kv, kv
        units = {0: kv}
        for k in range(1, nz):
            up = lax.ppermute(up, "z", [(s, s + 1) for s in range(k - 1, nz - 1)])
            down = lax.ppermute(down, "z", [(s + 1, s) for s in range(0, nz - k)])
            units[-k], units[k] = up, down
        kv_all = jnp.concatenate([units[k] for k in range(1 - nz, nz)], axis=0)
        base = (nz - 1 - z) * n
    else:
        kv_all = lax.all_gather(kv, "z", axis=0, tiled=True)
        base = 0

    plane_rows = lax.dynamic_slice_in_dim(everyone, z * ny, ny, axis=0)
    plane_rows = plane_rows.reshape(n, SELECTION_COUNT + 2)
    order = me ^ jnp.arange(n, dtype=jnp.int32)
    plane_rows = plane_rows[order]
    live = plane_rows[:, SELECTION_COUNT]
    chosen = plane_rows[:, :SELECTION_COUNT]
    chosen = jnp.where(jnp.arange(SELECTION_COUNT)[None] < live[:, None], chosen, chosen[:, :1])
    table = jnp.concatenate([live[:, None], slots[chosen] + base], axis=1)

    outs = [None] * n
    for d in reversed(range(n)):
        o = attend(table, q_parts[d], kv_all, d, groups)
        if d:
            o = lax.ppermute(o, plane, [(s, s ^ d) for s in range(n)])
        outs[d] = o
    return place(me, outs)


def solution(mesh):
    head = mesh.shape["head"]
    ny = KV_HEADS // head
    nz = mesh.shape["seq"] // ny
    grid = Mesh(mesh.devices.reshape(nz, ny, head), ("z", "y", "head"))
    rows = P(("z", "y", "head"), None)
    seq = ("z", "y")
    return jax.shard_map(
        body,
        mesh=grid,
        in_specs=(rows, rows, rows, P(seq, None), P(seq), P(seq)),
        out_specs=rows,
        check_vma=False,
    )
```

```python
import functools
import math

import jax
import jax.numpy as jnp
from jax import lax
from jax.experimental import pallas as pl
from jax.experimental.pallas import tpu as pltpu
from jax.sharding import Mesh
from jax.sharding import PartitionSpec as P

KV_HEADS = 8
HEAD_SIZE = 128
BLOCK_ROWS = 128
SELECTION_COUNT = 8
CHAIN_MAX = 4
CHUNK_HEADS = 4
BLOCKS_PER_CALL = 2
NEG = -1e30
VMEM_LIMIT = 24 * 1024 * 1024


def attend_kernel(tab_ref, *refs, ds, groups):
    nq = len(ds)
    q_refs, (k_ref, v_ref), o_refs = refs[:nq], refs[nq : nq + 2], refs[nq + 2 : 2 * nq + 2]
    kc_ref, vc_ref, s_ref = refs[2 * nq + 2 :]
    rows = CHUNK_HEADS * BLOCK_ROWS
    c = math.log2(math.e) / math.sqrt(HEAD_SIZE)
    block = (BLOCK_ROWS, HEAD_SIZE)
    qpos = lax.broadcasted_iota(jnp.int32, (CHUNK_HEADS, BLOCK_ROWS, BLOCK_ROWS), 1)
    kpos = lax.broadcasted_iota(jnp.int32, (CHUNK_HEADS, BLOCK_ROWS, BLOCK_ROWS), 2)
    tri = (kpos <= qpos).reshape(rows, BLOCK_ROWS)

    def gather(t):
        d = ds[t]
        count = tab_ref[d, 0]
        own = k_ref[tab_ref[d, 1]]
        first = jnp.broadcast_to(own[0:1, :], block)
        for e in range(SELECTION_COUNT):
            at = slice(e * BLOCK_ROWS, (e + 1) * BLOCK_ROWS)
            live = e < count
            pos = tab_ref[d, 1 + e]
            kc_ref[t, at, :] = jnp.where(live, k_ref[pos], first) if e else own
            vc_ref[t, at, :HEAD_SIZE] = jnp.where(live, v_ref[pos], jnp.zeros(block, jnp.bfloat16))
            vc_ref[t, at, HEAD_SIZE:] = jnp.where(
                live, jnp.ones(block, jnp.bfloat16), jnp.zeros(block, jnp.bfloat16)
            )

    def score(t, h, slot):
        q = jnp.concatenate(
            [
                q_refs[t][:, m * HEAD_SIZE : (m + 1) * HEAD_SIZE]
                for m in range(h * CHUNK_HEADS, (h + 1) * CHUNK_HEADS)
            ],
            axis=0,
        )
        s = lax.dot_general(
            q, kc_ref[t], (((1,), (1,)), ((), ())), preferred_element_type=jnp.float32
        )
        s_ref[slot, :, :BLOCK_ROWS] = jnp.where(tri, s[:, :BLOCK_ROWS], NEG)
        s_ref[slot, :, BLOCK_ROWS:] = s[:, BLOCK_ROWS:]

    def mix(t, h, slot):
        s = s_ref[slot]
        top = s[:, :BLOCK_ROWS]
        for e in range(1, SELECTION_COUNT):
            top = jnp.maximum(top, s[:, e * BLOCK_ROWS : (e + 1) * BLOCK_ROWS])
        shift = jnp.max(top, axis=1, keepdims=True) * c
        w = jnp.exp2(s * c - shift).astype(jnp.bfloat16)
        acc = jnp.dot(w, vc_ref[t], preferred_element_type=jnp.float32)
        out = (acc[:, :HEAD_SIZE] / acc[:, HEAD_SIZE:]).astype(jnp.bfloat16)
        for m in range(CHUNK_HEADS):
            col = (h * CHUNK_HEADS + m) * HEAD_SIZE
            o_refs[t][:, col : col + HEAD_SIZE] = out[m * BLOCK_ROWS : (m + 1) * BLOCK_ROWS]

    work = [(t, h) for t in range(nq) for h in range(groups // CHUNK_HEADS)]
    for t in range(nq):
        gather(t)
    score(*work[0], 0)
    for i in range(len(work)):
        if i + 1 < len(work):
            score(*work[i + 1], (i + 1) % 2)
        mix(*work[i], i % 2)


def attend(table, qs, keys, values, ds, groups):
    nq = len(ds)
    span = SELECTION_COUNT * BLOCK_ROWS
    vmem = pl.BlockSpec(memory_space=pltpu.VMEM)
    return pl.pallas_call(
        functools.partial(attend_kernel, ds=ds, groups=groups),
        out_shape=[jax.ShapeDtypeStruct(q.shape, q.dtype) for q in qs],
        in_specs=[pl.BlockSpec(memory_space=pltpu.SMEM)] + [vmem] * (nq + 2),
        out_specs=[vmem] * nq,
        scratch_shapes=[
            pltpu.VMEM((nq, span, HEAD_SIZE), jnp.bfloat16),
            pltpu.VMEM((nq, span, 2 * HEAD_SIZE), jnp.bfloat16),
            pltpu.VMEM((2, CHUNK_HEADS * BLOCK_ROWS, span), jnp.float32),
        ],
        compiler_params=pltpu.CompilerParams(vmem_limit_bytes=VMEM_LIMIT),
        name="attend",
    )(table, *qs, keys, values)


def sort_kernel(me_ref, *refs):
    n = len(refs) - 2
    for d in range(n):
        at = me_ref[0] ^ d
        refs[n][at] = refs[d][0]
        refs[n + 1][at] = refs[d][1]


def sort_pieces(me, pieces):
    n = len(pieces)
    vmem = pl.BlockSpec(memory_space=pltpu.VMEM)
    unit = jax.ShapeDtypeStruct((n,) + pieces[0].shape[1:], pieces[0].dtype)
    return pl.pallas_call(
        sort_kernel,
        out_shape=[unit, unit],
        in_specs=[pl.BlockSpec(memory_space=pltpu.SMEM)] + [vmem] * n,
        out_specs=[vmem, vmem],
        compiler_params=pltpu.CompilerParams(vmem_limit_bytes=VMEM_LIMIT),
        name="sort_pieces",
    )(me.reshape(1), *pieces)


def collect_kernel(z_ref, *refs, nz):
    n = len(refs) - 1
    out = refs[n]
    size = refs[0].shape[0]
    for i in range(n):
        at = z_ref[0] + i - (nz - 1)

        @pl.when(jnp.logical_and(at >= 0, at < nz))
        def _():
            for j in range(size):
                out[at * size + j] = refs[i][j]


def collect(z, units, nz):
    n = len(units)
    vmem = pl.BlockSpec(memory_space=pltpu.VMEM)
    return pl.pallas_call(
        functools.partial(collect_kernel, nz=nz),
        out_shape=jax.ShapeDtypeStruct(
            (nz * units[0].shape[0],) + units[0].shape[1:], units[0].dtype
        ),
        in_specs=[pl.BlockSpec(memory_space=pltpu.SMEM)] + [vmem] * n,
        out_specs=vmem,
        compiler_params=pltpu.CompilerParams(vmem_limit_bytes=VMEM_LIMIT),
        name="collect",
    )(z.reshape(1), *units)


def place_kernel(me_ref, *refs):
    n = len(refs) - 2
    out, sems = refs[n], refs[n + 1]
    width = refs[0].shape[1]
    copies = []
    for d in range(n):
        col = pl.multiple_of((me_ref[0] ^ d) * width, width)
        copies.append(pltpu.make_async_copy(refs[d], out.at[:, pl.ds(col, width)], sems.at[d]))
    for c in copies:
        c.start()
    for c in copies:
        c.wait()


def place(me, parts):
    n = len(parts)
    rows, width = parts[0].shape
    return pl.pallas_call(
        place_kernel,
        out_shape=jax.ShapeDtypeStruct((rows, n * width), parts[0].dtype),
        in_specs=[pl.BlockSpec(memory_space=pltpu.SMEM)]
        + [pl.BlockSpec(memory_space=pltpu.VMEM)] * n,
        out_specs=pl.BlockSpec(memory_space=pl.ANY),
        scratch_shapes=[pltpu.SemaphoreType.DMA((n,))],
        compiler_params=pltpu.CompilerParams(vmem_limit_bytes=VMEM_LIMIT),
        name="place",
    )(me.reshape(1), *parts)


def body(queries, keys, values, selected, counts, block_slot):
    plane = ("y", "head")
    nz = lax.axis_size("z")
    ny = lax.axis_size("y")
    nh = lax.axis_size("head")
    n = ny * nh
    z = lax.axis_index("z")
    me = lax.axis_index("y") * nh + lax.axis_index("head")
    width = queries.shape[1] // n
    groups = width // HEAD_SIZE

    def swap(x, d):
        return lax.ppermute(x, plane, [(s, s ^ d) for s in range(n)])

    pieces = []
    for d in range(n):
        at = (me ^ d) * HEAD_SIZE
        piece = jnp.stack(
            [lax.dynamic_slice_in_dim(x, at, HEAD_SIZE, axis=1) for x in (keys, values)]
        )
        if d:
            piece = swap(piece, d)
        pieces.append(piece)
    units = sort_pieces(me, pieces)

    gathered = []
    if nz <= CHAIN_MAX:
        up, down = list(units), list(units)
        runs = [{0: u} for u in units]
        for k in range(1, nz):
            for w in range(2):
                up[w] = lax.ppermute(up[w], "z", [(s, s + 1) for s in range(k - 1, nz - 1)])
                down[w] = lax.ppermute(down[w], "z", [(s + 1, s) for s in range(0, nz - k)])
                runs[w][-k], runs[w][k] = up[w], down[w]
        gathered = [collect(z, [r[k] for k in range(1 - nz, nz)], nz) for r in runs]
    else:
        gathered = [lax.all_gather(u, "z", axis=0, tiled=True) for u in units]

    q_parts = []
    for d in range(n):
        part = lax.dynamic_slice_in_dim(queries, (me ^ d) * width, width, axis=1)
        if d:
            part = swap(part, d)
        q_parts.append(part)

    mine = jnp.concatenate([selected, counts[:, None], block_slot[:, None]], axis=1)
    shards = nz * ny
    everyone = lax.all_to_all(
        jnp.broadcast_to(mine[None], (shards,) + mine.shape),
        ("z", "y"), split_axis=0, concat_axis=0, tiled=True,
    )
    slots = everyone[:, :, SELECTION_COUNT + 1].reshape(-1)
    plane_rows = lax.dynamic_slice_in_dim(everyone, z * ny, ny, axis=0)
    plane_rows = plane_rows.reshape(n, SELECTION_COUNT + 2)
    order = me ^ jnp.arange(n, dtype=jnp.int32)
    plane_rows = plane_rows[order]
    live = plane_rows[:, SELECTION_COUNT]
    table = jnp.concatenate([live[:, None], slots[plane_rows[:, :SELECTION_COUNT]]], axis=1)

    outs = [None] * n
    for top in range(n - 1, -1, -BLOCKS_PER_CALL):
        ds = list(range(top, max(top - BLOCKS_PER_CALL, -1), -1))
        got = attend(table, [q_parts[d] for d in ds], *gathered, ds, groups)
        for d, o in zip(ds, got):
            outs[d] = swap(o, d) if d else o
    return place(me, outs)


def solution(mesh):
    head = mesh.shape["head"]
    ny = KV_HEADS // head
    nz = mesh.shape["seq"] // ny
    grid = Mesh(mesh.devices.reshape(nz, ny, head), ("z", "y", "head"))
    rows = P(("z", "y", "head"), None)
    seq = ("z", "y")

    return jax.shard_map(
        body,
        mesh=grid,
        in_specs=(rows, rows, rows, P(seq, None), P(seq), P(seq)),
        out_specs=rows,
        check_vma=False,
    )
```
